128 devices in a mesh: left: 32 (over z, y_lo, x), right: 4 (over y_hi, core).
Axes of the slice: x: 4, y: 4 (y_hi: 2, y_lo: 2; y = y_hi * 2 + y_lo), z: 4, core: 2. Of those that a mesh axis runs over, the one named last changes fastest.
Arguments:
- density: float32 [512, 512, 2048], P(None, 'left', 'right'), may hold values from -6 to 6
- symbol_x: float32 [512], replicated, may hold values from 0.3 to 3
- symbol_y: float32 [512], replicated, may hold values from 0.3 to 3
- symbol_z: float32 [2048], replicated, may hold values from 0.3 to 3
Outputs:
- spectrum: float32 [512, 512, 2048], P('left', 'right')
The draws below stay inside these ranges and needn't reach their ends.
All inputs are finite; a program needn't handle non-finite values.
Results may differ from the reference program's by a relative error of at most 0.00007.
Values sent between devices are 32-bit elements; how exact they have to be, the bound alone decides.
No kernel may reach another device: no remote copies, remote signals or barrier semaphores. Data moves between devices by JAX's collectives and lax.ppermute only.
A program may use at most 192 MiB of HBM per device.

```python
import jax
import jax.numpy as jnp
from jax import lax

GRID_X = 512
GRID_Y = 512
GRID_Z = 2048


def level_of(rng, shape, split, smallest, high):
    def one(dim, parts):
        steps = jax.random.uniform(jax.random.fold_in(jax.random.fold_in(rng, 6), dim), (parts,), jnp.float32, smallest / len(split), high / len(split))
        return jnp.repeat(jnp.exp(steps), shape[dim] // parts).reshape((-1,) + (1,) * (len(shape) - dim - 1))

    level = one(*split[0])
    for cut in split[1:]:
        level = level * one(*cut)
    return level


def centred(key, shape, scale, most, pieces=(), kind=jnp.bfloat16):
    level = level_of(key, shape, pieces, -0.22, 0.18) if pieces else 1.0
    array = jax.random.normal(key, shape, jnp.float32) * scale * level
    return jnp.minimum(jnp.maximum(array, -most), most).astype(kind)


def setup_inputs(seed: int = 0) -> dict:
    streams_of = jax.random.split(jax.random.key(seed), 5)
    density = centred(streams_of[0], (GRID_X, GRID_Y, GRID_Z), 1.0, 6.0, ((1, 32), (2, 4)), jnp.float32)
    symbol_x = jnp.clip(jax.random.uniform(streams_of[1], (GRID_X,), jnp.float32, 0.3, 3.0), 0.3, 3.0)
    symbol_y = jnp.clip(jax.random.uniform(streams_of[2], (GRID_Y,), jnp.float32, 0.3, 3.0), 0.3, 3.0)
    symbol_z = jnp.clip(jax.random.uniform(streams_of[3], (GRID_Z,), jnp.float32, 0.3, 3.0), 0.3, 3.0)
    return {"density": density, "symbol_x": symbol_x, "symbol_y": symbol_y, "symbol_z": symbol_z}


def mode_table(count):
    rank = jnp.arange(count)
    angle = 2.0 * jnp.pi / count * (rank[:, None] * rank[None, :] % count).astype(jnp.float32)
    return (jnp.cos(angle) + jnp.sin(angle)) * count ** (-0.5)

def transform_dim(values, dim):
    moved = jnp.tensordot(values, mode_table(values.shape[dim]), axes=([dim], [0]), precision=lax.Precision.HIGHEST)
    return jnp.moveaxis(moved, -1, dim)

def reference(density, symbol_x, symbol_y, symbol_z):
    spectrum = density
    spectrum = transform_dim(spectrum, 0)
    spectrum = transform_dim(spectrum, 1)
    spectrum = transform_dim(spectrum, 2)
    symbol = symbol_x[:, None, None] + symbol_y[None, :, None] + symbol_z[None, None, :]
    spectrum = spectrum * lax.rsqrt(symbol)
    return spectrum
```

```python
import functools

import jax
import jax.numpy as jnp
import numpy as np
from jax import lax
from jax.experimental import pallas as pl
from jax.experimental.pallas import tpu as pltpu
from jax.sharding import PartitionSpec as P

CUTS = (0, 2, 7, 11, 14, 16)
F32 = jnp.float32
BF16 = jnp.bfloat16


def turns(rows, cols, count):
    return 2.0 * np.pi / count * (np.asarray(rows)[:, None] * np.asarray(cols)[None, :] % count)


def mode_rows(rows, cols, count):
    angle = turns(rows, cols, count)
    return ((np.cos(angle) + np.sin(angle)) * count**-0.5).astype(np.float32)


def np_halves(table):
    high = table.astype(jnp.bfloat16)
    low = (table - high.astype(np.float32)).astype(jnp.bfloat16)
    return jnp.asarray(high), jnp.asarray(low)


def halves(value):
    high = value.astype(BF16)
    return high, (value - high.astype(F32)).astype(BF16)


def dot(a, b):
    return jnp.dot(a, b, preferred_element_type=F32)


def x_kernel(values, even_high, even_low, odd_high, odd_low, out):
    count, rows, lanes = values.shape
    half = count // 2
    flat = values.reshape(count * rows, lanes)
    flat_out = out.reshape(count * rows, lanes)
    for row in range(0, rows, 2):
        first = [flat[pl.ds(row + k, half, stride=rows), :] for k in range(2)]
        second = [flat[pl.ds(half * rows + row + k, half, stride=rows), :] for k in range(2)]
        first = jnp.concatenate(first, axis=1)
        second = jnp.concatenate(second, axis=1)
        for parity, mixed, high, low in (
            (0, first + second, even_high, even_low),
            (1, first - second, odd_high, odd_low),
        ):
            mixed_high, mixed_low = halves(mixed)
            done = dot(high[...], mixed_high) + dot(low[...], mixed_high) + dot(high[...], mixed_low)
            for k in range(2):
                flat_out[pl.ds(parity * rows + row + k, half, stride=2 * rows), :] = done[:, k * lanes : (k + 1) * lanes]


def fold_tables(count):
    first = np.arange(count // 2)
    even = mode_rows(np.arange(0, count, 2), first, count)
    odd = mode_rows(np.arange(1, count, 2), first, count)
    return np_halves(even) + np_halves(odd)


def x_modes(density):
    nx, ny, nz = density.shape
    half = nx // 2
    rows, lanes = 8, 128
    block = pl.BlockSpec((nx, rows, lanes), lambda i, k: (0, i, k))
    fixed = pl.BlockSpec((half, half), lambda i, k: (0, 0))
    return pl.pallas_call(
        x_kernel,
        grid=(ny // rows, nz // lanes),
        in_specs=[block] + [fixed] * 4,
        out_specs=block,
        out_shape=jax.ShapeDtypeStruct((nx, ny, nz), F32),
        name="x_modes",
    )(density, *fold_tables(nx))


def y_kernel(own, values, *rest, right):
    tables, outs = rest[: 2 * right], rest[2 * right :]
    parts, _, part, nz = values.shape
    share = outs[0].shape[1]
    high = jnp.concatenate([table[...] for table in tables[:right]], axis=0)
    low = jnp.concatenate([table[...] for table in tables[right:]], axis=0)
    full_high, full_low = halves(values[...].reshape(parts * part, nz))
    done = dot(high, full_high) + dot(low, full_high) + dot(high, full_low)
    for k, out in enumerate(outs):
        out[0] = done[k * share : (k + 1) * share]


def y_modes(values, own, lo, hi, right):
    parts, _, part, nz = values.shape
    ny = parts * part
    share = ny // right
    tables = np_halves(mode_rows(np.arange(ny), np.arange(ny), ny))
    pick = [pl.BlockSpec((share, ny), lambda j, own, k=k: (own[0] ^ k, 0)) for k in range(right)]
    return pl.pallas_call(
        functools.partial(y_kernel, right=right),
        grid_spec=pltpu.PrefetchScalarGridSpec(
            num_scalar_prefetch=1,
            grid=(hi - lo,),
            in_specs=[pl.BlockSpec((parts, 1, part, nz), lambda j, own: (0, lo + j, 0, 0))] + pick * 2,
            out_specs=[pl.BlockSpec((1, share, nz), lambda j, own: (j, 0, 0))] * right,
        ),
        out_shape=[jax.ShapeDtypeStruct((hi - lo, share, nz), F32)] * right,
        name="y_modes",
    )(own, values, *[table for table in tables for _ in range(right)])


def z_kernel(part_x, high, low, part_y, symbol_z, *rest, lo, count, summed, last):
    values = rest[:count]
    out, mine = rest[-2:]
    own, share, width = values[0].shape
    rows = own * share

    @pl.when(pl.program_id(0) == 0)
    def _():
        for r in range(count):
            value_high, value_low = halves(values[r][...].reshape(rows, width))
            mine[:rows, r * width : (r + 1) * width] = value_high
            mine[rows:, r * width : (r + 1) * width] = value_low

    both = dot(mine[...], high[...])
    done = both[:rows] + both[rows:] + dot(mine[:rows], low[...])
    for j in range(own):
        result = done[j * share : (j + 1) * share]
        if summed:
            result = result + rest[count][j]
        if last:
            result = result * lax.rsqrt(part_x[lo + j] + part_y[...] + symbol_z[...])
        out[j] = result


def z_modes(values, places, tables, symbols, lo, sums=None, out=None, last=True):
    count = len(values)
    own, share, width = values[0].shape
    part_x, part_y, symbol_z = symbols
    nz = symbol_z.shape[1]
    lanes = 256
    cols = pl.BlockSpec((count * width, lanes), lambda n: (places[0] // count, n))
    sum_block = pl.BlockSpec((own, share, lanes), lambda n: (0, 0, n))
    in_specs = [
        pl.BlockSpec(memory_space=pltpu.SMEM),
        cols,
        cols,
        pl.BlockSpec((share, 1), lambda n: (0, 0)),
        pl.BlockSpec((1, lanes), lambda n: (0, n)),
    ] + [pl.BlockSpec((own, share, width), lambda n: (0, 0, 0))] * count
    args = [part_x, *tables, part_y, symbol_z, *values]
    if sums is not None:
        in_specs.append(sum_block)
        args.append(sums)
    aliases = {}
    if out is not None:
        aliases = {len(args): 0}
        in_specs.append(pl.BlockSpec(memory_space=pl.ANY))
        args.append(out)
    full_block = pl.BlockSpec((pl.Element(own), pl.Element(share), pl.Element(lanes)), lambda n: (lo, 0, n * lanes))
    return pl.pallas_call(
        functools.partial(z_kernel, lo=lo, count=count, summed=sums is not None, last=last),
        grid=(nz // lanes,),
        in_specs=in_specs,
        out_specs=full_block if last else sum_block,
        out_shape=jax.ShapeDtypeStruct((part_x.shape[0] if last else own, share, nz), F32),
        scratch_shapes=[pltpu.VMEM((2 * own * share, count * width), BF16)],
        input_output_aliases=aliases,
        name="z_modes",
    )(*args)


def run_halves(table):
    high = lax.reduce_precision(table, 8, 7)
    return high.astype(BF16), (table - high).astype(BF16)


def angles(rows, cols, count):
    return 2.0 * jnp.pi / count * (rows[:, None] * cols[None, :] % count).astype(F32)


def z_tables(nz, right, own, zero):
    step = 64
    share = nz // right
    cols = jnp.arange(nz) + zero
    rank = jnp.arange(0, nz, step) + zero
    coarse = angles(((rank // share) ^ own) * share + rank % share, cols, nz)
    fine = angles(jnp.arange(step), cols, nz)
    cos, sin = jnp.cos(fine) * nz**-0.5, jnp.sin(fine) * nz**-0.5
    near, back, cos, sin = lax.optimization_barrier((cos + sin, cos - sin, jnp.cos(coarse), jnp.sin(coarse)))
    high, low = run_halves(cos[:, None, :] * near[None] + sin[:, None, :] * back[None])
    return high.reshape(nz, nz), low.reshape(nz, nz)


def per_device(density, symbol_x, symbol_y, symbol_z):
    left = lax.axis_size("left")
    right = lax.axis_size("right")
    nx, ny_part, nz_part = density.shape
    share_x = nx // left
    share_y = ny_part * left // right
    a = x_modes(density).reshape(left, share_x, ny_part, nz_part)
    at_left = lax.axis_index("left").astype(jnp.int32)
    at_right = lax.axis_index("right").astype(jnp.int32)[None]
    a, at_left, at_right = lax.optimization_barrier((a, at_left, at_right))
    a = lax.all_to_all(a, "left", split_axis=0, concat_axis=0, tiled=True)
    sent = []
    for c, (lo, hi) in enumerate(zip(CUTS, CUTS[1:])):
        b = y_modes(a, at_right, lo, hi, right)
        a, mine, at_left, zero = lax.optimization_barrier((a, b[0], at_left, jnp.int32(0)))
        met = [mine]
        for k in range(1, right):
            met.append(lax.ppermute(b[k], "right", [(r, r ^ k) for r in range(right)]))
        sent.append(met)
        if c == 1:
            at = at_right[0] + zero
            tables = z_tables(nz_part * right, right, at, zero)
            part_x = lax.dynamic_slice_in_dim(symbol_x, at_left * share_x, share_x)
            part_y = lax.dynamic_slice_in_dim(symbol_y, at * share_y, share_y)[:, None]
            symbols = (part_x, part_y, symbol_z[None])
    out = None
    for c, (lo, hi) in enumerate(zip(CUTS, CUTS[1:])):
        met = sent[c]
        if hi < share_x:
            out = z_modes(met, range(right), tables, symbols, lo, out=out)
        else:
            half = right // 2
            sums = z_modes(met[:half], range(half), tables, symbols, lo, last=False)
            out = z_modes(met[half:], range(half, right), tables, symbols, lo, sums=sums, out=out)
    return out


def solution(mesh):
    return jax.shard_map(
        per_device,
        mesh=mesh,
        in_specs=(P(None, "left", "right"), P(), P(), P()),
        out_specs=P("left", "right", None),
        check_vma=False,
    )
```

```python
import functools

import jax
import jax.numpy as jnp
import numpy as np
from jax import lax
from jax.experimental import pallas as pl
from jax.experimental.pallas import tpu as pltpu
from jax.sharding import PartitionSpec as P

CUTS = (0, 2, 7, 11, 14, 16)
F32 = jnp.float32
BF16 = jnp.bfloat16


def turns(rows, cols, count):
    return 2.0 * np.pi / count * (np.asarray(rows)[:, None] * np.asarray(cols)[None, :] % count)


def mode_rows(rows, cols, count):
    angle = turns(rows, cols, count)
    return ((np.cos(angle) + np.sin(angle)) * count**-0.5).astype(np.float32)


def np_halves(table):
    high = table.astype(jnp.bfloat16)
    low = (table - high.astype(np.float32)).astype(jnp.bfloat16)
    return jnp.asarray(high), jnp.asarray(low)


def halves(value):
    high = value.astype(BF16)
    return high, (value - high.astype(F32)).astype(BF16)


def dot(a, b):
    return jnp.dot(a, b, preferred_element_type=F32)


def x_kernel(values, tables, out):
    count, rows, lanes = values.shape
    half = count // 2
    flat = values.reshape(count * rows, lanes)
    z = pl.ds(pl.multiple_of(pl.program_id(1) * lanes, lanes), lanes)
    results = {}
    for row in range(0, rows, 2):
        first = [flat[pl.ds(row + k, half, stride=rows), :] for k in range(2)]
        second = [flat[pl.ds(half * rows + row + k, half, stride=rows), :] for k in range(2)]
        first = jnp.concatenate(first, axis=1)
        second = jnp.concatenate(second, axis=1)
        for parity, mixed, high, low in (
            (0, first + second, tables[0], tables[1]),
            (1, first - second, tables[2], tables[3]),
        ):
            mixed_high, mixed_low = halves(mixed)
            both = dot(jnp.concatenate([high, low], axis=0), mixed_high)
            done = both[:half] + both[half:] + dot(high, mixed_low)
            for k in range(2):
                results[parity, row + k] = done[:, k * lanes : (k + 1) * lanes]
    for parity in range(2):
        stack = jnp.stack([results[parity, row] for row in range(rows)], axis=0)
        out.reshape(half, 2, *out.shape[1:])[:, parity, pl.ds(pl.multiple_of(pl.program_id(0) * rows, rows), rows), z] = jnp.swapaxes(stack, 0, 1)


def fold_tables(count):
    first = np.arange(count // 2)
    even = mode_rows(np.arange(0, count, 2), first, count)
    odd = mode_rows(np.arange(1, count, 2), first, count)
    return jnp.stack(np_halves(even) + np_halves(odd))


def x_modes(density):
    nx, ny, nz = density.shape
    half = nx // 2
    rows, lanes = 8, 128
    block = pl.BlockSpec((nx, rows, lanes), lambda i, k: (0, i, k))
    return pl.pallas_call(
        x_kernel,
        grid=(ny // rows, nz // lanes),
        in_specs=[block, pl.BlockSpec((4, half, half), lambda i, k: (0, 0, 0))],
        out_specs=pl.BlockSpec(memory_space=pltpu.VMEM),
        out_shape=pltpu.VMEM((nx, ny, nz), F32),
        compiler_params=pltpu.CompilerParams(vmem_limit_bytes=43 * 2**20),
        name="x_modes",
    )(density, fold_tables(nx))


def y_kernel(own, values, *rest, right):
    tables, outs = rest[: 2 * right], rest[2 * right :]
    parts, _, part, nz = values.shape
    share = outs[0].shape[1]
    high = jnp.concatenate([table[...] for table in tables[:right]], axis=0)
    low = jnp.concatenate([table[...] for table in tables[right:]], axis=0)
    full_high, full_low = halves(values[...].reshape(parts * part, nz))
    done = dot(high, full_high) + dot(low, full_high) + dot(high, full_low)
    for k, out in enumerate(outs):
        out[0] = done[k * share : (k + 1) * share]


def y_modes(values, own, lo, hi, right):
    parts, _, part, nz = values.shape
    ny = parts * part
    share = ny // right
    tables = np_halves(mode_rows(np.arange(ny), np.arange(ny), ny))
    pick = [pl.BlockSpec((share, ny), lambda j, own, k=k: (own[0] ^ k, 0)) for k in range(right)]
    return pl.pallas_call(
        functools.partial(y_kernel, right=right),
        grid_spec=pltpu.PrefetchScalarGridSpec(
            num_scalar_prefetch=1,
            grid=(hi - lo,),
            in_specs=[pl.BlockSpec((parts, 1, part, nz), lambda j, own: (0, lo + j, 0, 0))] + pick * 2,
            out_specs=[pl.BlockSpec((1, share, nz), lambda j, own: (j, 0, 0))] * right,
        ),
        out_shape=[jax.ShapeDtypeStruct((hi - lo, share, nz), F32)] * right,
        name="y_modes",
    )(own, values, *[table for table in tables for _ in range(right)])


def z_kernel(part_x, high, low, part_y, symbol_z, *rest, lo, count, summed, last):
    values = rest[:count]
    out, mine = rest[-2:]
    own, share, width = values[0].shape
    rows = own * share

    @pl.when(pl.program_id(0) == 0)
    def _():
        for r in range(count):
            value_high, value_low = halves(values[r][...].reshape(rows, width))
            mine[:rows, r * width : (r + 1) * width] = value_high
            mine[rows:, r * width : (r + 1) * width] = value_low

    both = dot(mine[...], high[...])
    done = both[:rows] + both[rows:] + dot(mine[:rows], low[...])
    for j in range(own):
        result = done[j * share : (j + 1) * share]
        if summed:
            result = result + rest[count][j]
        if last:
            result = result * lax.rsqrt(part_x[lo + j] + part_y[...] + symbol_z[...])
        out[j] = result


def z_modes(values, places, tables, symbols, lo, sums=None, out=None, last=True):
    count = len(values)
    own, share, width = values[0].shape
    part_x, part_y, symbol_z = symbols
    nz = symbol_z.shape[1]
    lanes = 256 if count > 1 else 512
    cols = pl.BlockSpec((count * width, lanes), lambda n: (places[0] // count, n))
    sum_block = pl.BlockSpec((own, share, lanes), lambda n: (0, 0, n))
    in_specs = [
        pl.BlockSpec(memory_space=pltpu.SMEM),
        cols,
        cols,
        pl.BlockSpec((share, 1), lambda n: (0, 0)),
        pl.BlockSpec((1, lanes), lambda n: (0, n)),
    ] + [pl.BlockSpec((own, share, width), lambda n: (0, 0, 0))] * count
    args = [part_x, *tables, part_y, symbol_z, *values]
    if sums is not None:
        in_specs.append(sum_block)
        args.append(sums)
    aliases = {}
    if out is not None:
        aliases = {len(args): 0}
        in_specs.append(pl.BlockSpec(memory_space=pl.ANY))
        args.append(out)
    full_block = pl.BlockSpec((pl.Element(own), pl.Element(share), pl.Element(lanes)), lambda n: (lo, 0, n * lanes))
    return pl.pallas_call(
        functools.partial(z_kernel, lo=lo, count=count, summed=sums is not None, last=last),
        grid=(nz // lanes,),
        in_specs=in_specs,
        out_specs=full_block if last else sum_block,
        out_shape=jax.ShapeDtypeStruct((part_x.shape[0] if last else own, share, nz), F32),
        scratch_shapes=[pltpu.VMEM((2 * own * share, count * width), BF16)],
        input_output_aliases=aliases,
        name="z_modes",
    )(*args)


def run_halves(table):
    high = lax.reduce_precision(table, 8, 7)
    return high.astype(BF16), (table - high).astype(BF16)


def angles(rows, cols, count):
    return 2.0 * jnp.pi / count * (rows[:, None] * cols[None, :] % count).astype(F32)


def z_tables(nz, right, own, zero):
    step = 64
    share = nz // right
    cols = jnp.arange(nz) + zero
    rank = jnp.arange(0, nz, step) + zero
    coarse = angles(((rank // share) ^ own) * share + rank % share, cols, nz)
    fine = angles(jnp.arange(step), cols, nz)
    cos, sin = jnp.cos(fine) * nz**-0.5, jnp.sin(fine) * nz**-0.5
    near, back, cos, sin = lax.optimization_barrier((cos + sin, cos - sin, jnp.cos(coarse), jnp.sin(coarse)))
    high, low = run_halves(cos[:, None, :] * near[None] + sin[:, None, :] * back[None])
    return high.reshape(nz, nz), low.reshape(nz, nz)


def per_device(density, symbol_x, symbol_y, symbol_z):
    left = lax.axis_size("left")
    right = lax.axis_size("right")
    nx, ny_part, nz_part = density.shape
    share_x = nx // left
    share_y = ny_part * left // right
    a = x_modes(density).reshape(left, share_x, ny_part, nz_part)
    at_left = lax.axis_index("left").astype(jnp.int32)
    at_right = lax.axis_index("right").astype(jnp.int32)[None]
    a, at_left, at_right = lax.optimization_barrier((a, at_left, at_right))
    a = lax.all_to_all(a, "left", split_axis=0, concat_axis=0, tiled=True)
    sent = []
    for c, (lo, hi) in enumerate(zip(CUTS, CUTS[1:])):
        b = y_modes(a, at_right, lo, hi, right)
        a, mine, at_left, zero = lax.optimization_barrier((a, b[0], at_left, jnp.int32(0)))
        met = [mine]
        for k in range(1, right):
            met.append(lax.ppermute(b[k], "right", [(r, r ^ k) for r in range(right)]))
        sent.append(met)
        if c == 1:
            at = at_right[0] + zero
            tables = z_tables(nz_part * right, right, at, zero)
            part_x = lax.dynamic_slice_in_dim(symbol_x, at_left * share_x, share_x)
            part_y = lax.dynamic_slice_in_dim(symbol_y, at * share_y, share_y)[:, None]
            symbols = (part_x, part_y, symbol_z[None])
    out = None
    for c, (lo, hi) in enumerate(zip(CUTS, CUTS[1:])):
        met = sent[c]
        if hi < share_x:
            out = z_modes(met, range(right), tables, symbols, lo, out=out)
        else:
            half = right // 2
            sums = z_modes(met[:half], range(half), tables, symbols, lo, last=False)
            for k in range(half, right - 1):
                sums, out = lax.optimization_barrier((sums, out))
                sums = z_modes(met[k : k + 1], (k,), tables, symbols, lo, sums=sums, last=False)
            out = z_modes(met[-1:], (right - 1,), tables, symbols, lo, sums=sums, out=out)
    return out


def solution(mesh):
    return jax.shard_map(
        per_device,
        mesh=mesh,
        in_specs=(P(None, "left", "right"), P(), P(), P()),
        out_specs=P("left", "right", None),
        check_vma=False,
    )
```

```python
import functools

import jax
import jax.numpy as jnp
import numpy as np
from jax import lax
from jax.experimental import pallas as pl
from jax.experimental.pallas import tpu as pltpu
from jax.sharding import PartitionSpec as P

CUTS = (0, 1, 3, 8, 12, 14, 16)
F32 = jnp.float32
BF16 = jnp.bfloat16


def turns(rows, cols, count):
    return 2.0 * np.pi / count * (np.asarray(rows)[:, None] * np.asarray(cols)[None, :] % count)


def mode_rows(rows, cols, count):
    angle = turns(rows, cols, count)
    return ((np.cos(angle) + np.sin(angle)) * count**-0.5).astype(np.float32)


def np_halves(table):
    high = table.astype(jnp.bfloat16)
    low = (table - high.astype(np.float32)).astype(jnp.bfloat16)
    return jnp.asarray(high), jnp.asarray(low)


def halves(value):
    high = value.astype(BF16)
    return high, (value - high.astype(F32)).astype(BF16)


def dot(a, b):
    return jnp.dot(a, b, preferred_element_type=F32)


def x_kernel(values, tables, out):
    count, rows, lanes = values.shape
    half = count // 2
    flat = values.reshape(count * rows, lanes)
    z = pl.ds(pl.multiple_of(pl.program_id(1) * lanes, lanes), lanes)
    results = {}
    for row in range(0, rows, 2):
        first = [flat[pl.ds(row + k, half, stride=rows), :] for k in range(2)]
        second = [flat[pl.ds(half * rows + row + k, half, stride=rows), :] for k in range(2)]
        first = jnp.concatenate(first, axis=1)
        second = jnp.concatenate(second, axis=1)
        for parity, mixed, high, low in (
            (0, first + second, tables[0], tables[1]),
            (1, first - second, tables[2], tables[3]),
        ):
            mixed_high, mixed_low = halves(mixed)
            both = dot(jnp.concatenate([high, low], axis=0), mixed_high)
            done = both[:half] + both[half:] + dot(high, mixed_low)
            for k in range(2):
                results[parity, row + k] = done[:, k * lanes : (k + 1) * lanes]
    for parity in range(2):
        stack = jnp.stack([results[parity, row] for row in range(rows)], axis=0)
        out.reshape(half, 2, *out.shape[1:])[:, parity, pl.ds(pl.multiple_of(pl.program_id(0) * rows, rows), rows), z] = jnp.swapaxes(stack, 0, 1)


def fold_tables(count):
    first = np.arange(count // 2)
    even = mode_rows(np.arange(0, count, 2), first, count)
    odd = mode_rows(np.arange(1, count, 2), first, count)
    return jnp.stack(np_halves(even) + np_halves(odd))


def x_modes(density):
    nx, ny, nz = density.shape
    half = nx // 2
    rows, lanes = 8, 128
    block = pl.BlockSpec((nx, rows, lanes), lambda i, k: (0, i, k))
    return pl.pallas_call(
        x_kernel,
        grid=(ny // rows, nz // lanes),
        in_specs=[block, pl.BlockSpec((4, half, half), lambda i, k: (0, 0, 0))],
        out_specs=pl.BlockSpec(memory_space=pltpu.VMEM),
        out_shape=pltpu.VMEM((nx, ny, nz), F32),
        compiler_params=pltpu.CompilerParams(vmem_limit_bytes=43 * 2**20),
        name="x_modes",
    )(density, fold_tables(nx))


def y_kernel(own, values, *rest, right):
    tables, outs = rest[: 2 * right], rest[2 * right :]
    parts, _, part, nz = values.shape
    share = outs[0].shape[1]
    high = jnp.concatenate([table[...] for table in tables[:right]], axis=0)
    low = jnp.concatenate([table[...] for table in tables[right:]], axis=0)
    full_high, full_low = halves(values[...].reshape(parts * part, nz))
    done = dot(high, full_high) + dot(low, full_high) + dot(high, full_low)
    for k, out in enumerate(outs):
        out[0] = done[k * share : (k + 1) * share]


def y_modes(values, own, lo, hi, right):
    parts, _, part, nz = values.shape
    ny = parts * part
    share = ny // right
    tables = np_halves(mode_rows(np.arange(ny), np.arange(ny), ny))
    pick = [pl.BlockSpec((share, ny), lambda j, own, k=k: (own[0] ^ k, 0)) for k in range(right)]
    return pl.pallas_call(
        functools.partial(y_kernel, right=right),
        grid_spec=pltpu.PrefetchScalarGridSpec(
            num_scalar_prefetch=1,
            grid=(hi - lo,),
            in_specs=[pl.BlockSpec((parts, 1, part, nz), lambda j, own: (0, lo + j, 0, 0))] + pick * 2,
            out_specs=[pl.BlockSpec((1, share, nz), lambda j, own: (j, 0, 0))] * right,
        ),
        out_shape=[jax.ShapeDtypeStruct((hi - lo, share, nz), F32)] * right,
        name="y_modes",
    )(own, values, *[table for table in tables for _ in range(right)])


def z_kernel(part_x, high, low, part_y, symbol_z, *rest, lo, count, summed, last):
    values = rest[:count]
    out, mine = rest[-2:]
    own, share, width = values[0].shape
    rows = own * share

    @pl.when(pl.program_id(0) == 0)
    def _():
        for r in range(count):
            value_high, value_low = halves(values[r][...].reshape(rows, width))
            mine[:rows, r * width : (r + 1) * width] = value_high
            mine[rows:, r * width : (r + 1) * width] = value_low

    both = dot(mine[...], high[...])
    done = both[:rows] + both[rows:] + dot(mine[:rows], low[...])
    for j in range(own):
        result = done[j * share : (j + 1) * share]
        if summed:
            result = result + rest[count][j]
        if last:
            result = result * lax.rsqrt(part_x[lo + j] + part_y[...] + symbol_z[...])
        out[j] = result


def z_modes(values, places, tables, symbols, lo, sums=None, out=None, last=True):
    count = len(values)
    own, share, width = values[0].shape
    part_x, part_y, symbol_z = symbols
    nz = symbol_z.shape[1]
    lanes = 256 if count > 1 else 512
    cols = pl.BlockSpec((count * width, lanes), lambda n: (places[0] // count, n))
    sum_block = pl.BlockSpec((own, share, lanes), lambda n: (0, 0, n))
    in_specs = [
        pl.BlockSpec(memory_space=pltpu.SMEM),
        cols,
        cols,
        pl.BlockSpec((share, 1), lambda n: (0, 0)),
        pl.BlockSpec((1, lanes), lambda n: (0, n)),
    ] + [pl.BlockSpec((own, share, width), lambda n: (0, 0, 0))] * count
    args = [part_x, *tables, part_y, symbol_z, *values]
    if sums is not None:
        in_specs.append(sum_block)
        args.append(sums)
    aliases = {}
    if out is not None:
        aliases = {len(args): 0}
        in_specs.append(pl.BlockSpec(memory_space=pl.ANY))
        args.append(out)
    full_block = pl.BlockSpec((pl.Element(own), pl.Element(share), pl.Element(lanes)), lambda n: (lo, 0, n * lanes))
    return pl.pallas_call(
        functools.partial(z_kernel, lo=lo, count=count, summed=sums is not None, last=last),
        grid=(nz // lanes,),
        in_specs=in_specs,
        out_specs=full_block if last else sum_block,
        out_shape=jax.ShapeDtypeStruct((part_x.shape[0] if last else own, share, nz), F32),
        scratch_shapes=[pltpu.VMEM((2 * own * share, count * width), BF16)],
        input_output_aliases=aliases,
        compiler_params=pltpu.CompilerParams(vmem_limit_bytes=(59 if last and sums is None else 52) * 2**20),
        name="z_modes",
    )(*args)


def run_halves(table):
    high = lax.reduce_precision(table, 8, 7)
    return high.astype(BF16), (table - high).astype(BF16)


def angles(rows, cols, count):
    return 2.0 * jnp.pi / count * (rows[:, None] * cols[None, :] % count).astype(F32)


def z_tables(nz, right, own, zero):
    step = 64
    share = nz // right
    cols = jnp.arange(nz) + zero
    rank = jnp.arange(0, nz, step) + zero
    coarse = angles(((rank // share) ^ own) * share + rank % share, cols, nz)
    fine = angles(jnp.arange(step), cols, nz)
    cos, sin = jnp.cos(fine) * nz**-0.5, jnp.sin(fine) * nz**-0.5
    near, back, cos, sin = lax.optimization_barrier((cos + sin, cos - sin, jnp.cos(coarse), jnp.sin(coarse)))
    high, low = run_halves(cos[:, None, :] * near[None] + sin[:, None, :] * back[None])
    return high.reshape(nz, nz), low.reshape(nz, nz)


def per_device(density, symbol_x, symbol_y, symbol_z):
    left = lax.axis_size("left")
    right = lax.axis_size("right")
    nx, ny_part, nz_part = density.shape
    share_x = nx // left
    share_y = ny_part * left // right
    a = x_modes(density).reshape(left, share_x, ny_part, nz_part)
    at_left = lax.axis_index("left").astype(jnp.int32)
    at_right = lax.axis_index("right").astype(jnp.int32)[None]
    a, at_left, at_right = lax.optimization_barrier((a, at_left, at_right))
    a = lax.all_to_all(a, "left", split_axis=0, concat_axis=0, tiled=True)
    sent = []
    for c, (lo, hi) in enumerate(zip(CUTS, CUTS[1:])):
        b = y_modes(a, at_right, lo, hi, right)
        a, mine, at_left, zero = lax.optimization_barrier((a, b[0], at_left, jnp.int32(0)))
        met = [mine]
        for k in range(1, right):
            met.append(lax.ppermute(b[k], "right", [(r, r ^ k) for r in range(right)]))
        sent.append(met)
        if c == 2:
            at = at_right[0] + zero
            tables = z_tables(nz_part * right, right, at, zero)
            part_x = lax.dynamic_slice_in_dim(symbol_x, at_left * share_x, share_x)
            part_y = lax.dynamic_slice_in_dim(symbol_y, at * share_y, share_y)[:, None]
            symbols = (part_x, part_y, symbol_z[None])
    out = None
    for c, (lo, hi) in enumerate(zip(CUTS, CUTS[1:])):
        met = sent[c]
        if hi < share_x:
            out = z_modes(met, range(right), tables, symbols, lo, out=out)
        else:
            half = right // 2
            sums = z_modes(met[:half], range(half), tables, symbols, lo, last=False)
            for k in range(half, right - 1):
                sums, out = lax.optimization_barrier((sums, out))
                sums = z_modes(met[k : k + 1], (k,), tables, symbols, lo, sums=sums, last=False)
            out = z_modes(met[-1:], (right - 1,), tables, symbols, lo, sums=sums, out=out)
    return out


def solution(mesh):
    return jax.shard_map(
        per_device,
        mesh=mesh,
        in_specs=(P(None, "left", "right"), P(), P(), P()),
        out_specs=P("left", "right", None),
        check_vma=False,
    )
```
